32 devices in a mesh: bank: 4 (over x, core), zero: 8 (over z, y).
Axes of the slice: x: 2, y: 2, z: 4, core: 2. Of those that a mesh axis runs over, the one named last changes fastest.
Arguments:
- train_gate: float32 [128, 2048, 768], P('bank', 'zero'), may hold values from -0.1875 to 0.1875
- other_gate: bfloat16 [128, 2048, 768], P('bank', 'zero'), may hold values from -0.0625 to 0.0625
- train_up: float32 [128, 2048, 768], P('bank', 'zero'), may hold values from -0.1875 to 0.1875
- other_up: bfloat16 [128, 2048, 768], P('bank', 'zero'), may hold values from -0.0625 to 0.0625
- router_weight: float32 [2048, 128], P('zero', 'bank'), may hold values from -0.125 to 0.125
- router_gain: float32 [2048], P('zero'), may hold values from 0.25 to 1.75
Outputs:
- ready_gate: bfloat16 [128, 2048, 768], P('bank', None, 'zero')
- ready_up: bfloat16 [128, 2048, 768], P('bank', None, 'zero')
- scale_gate: float32 [128, 768], P('bank', 'zero')
- scale_up: float32 [128, 768], P('bank', 'zero')
- serve_router: bfloat16 [2048, 128], replicated
The draws below stay inside these ranges and needn't reach their ends.
All inputs are finite; a program needn't handle non-finite values. Where the reference program divides by a largest or mean magnitude, that divisor is 1e-20 or more.
Results may differ from the reference program's by a relative error of at most 0.001.
Values may be sent and summed in bfloat16 or wider, within the bound.
A program may use at most 256 MiB of HBM per device.

```python
import jax
import jax.numpy as jnp

EXPERTS = 128
D_MODEL = 2048
D_EXPERT = 768


def raised(array, rng, source, target, parts, factor):
    owner, partner = [(jnp.arange(array.shape[axis_at]) // (array.shape[axis_at] // parts)).reshape([-1 if axis == axis_at else 1 for axis in range(array.ndim)]) for axis_at in (source, target)]
    chosen = jax.random.permutation(rng, parts)[partner]
    strong = (owner == chosen) | (owner == (partner + parts // 2) % parts)
    return jnp.where(strong, factor * array, array)


def level_of(rng, extent, pieces, smallest, high):
    factor_of, own = 1.0, jax.random.fold_in(rng, 6)
    for position, blocks in pieces:
        draws = jnp.exp(jax.random.uniform(jax.random.fold_in(own, position), (blocks,), jnp.float32, smallest / len(pieces), high / len(pieces)))
        factor_of = factor_of * jnp.repeat(draws, extent[position] // blocks).reshape([-1 if axis == position else 1 for axis in range(len(extent))])
    return factor_of


def scatter_about(own_key, extent, scale, reach, split=(), dtype=jnp.bfloat16):
    loudness = level_of(own_key, extent, split, -0.22, 0.18) if split else 1.0
    entries = jax.random.normal(own_key, extent, jnp.float32) * scale * loudness
    return jnp.minimum(jnp.maximum(entries, -reach), reach).astype(dtype)


def heavy_noise(rng, dims, width, most, pieces, heavy, held_as=jnp.bfloat16):
    array = width * jax.random.normal(rng, dims, jnp.float32)
    if pieces:
        array = array * level_of(rng, dims, pieces, -0.22, 0.18)
    return jnp.clip(raised(array, jax.random.fold_in(rng, 3), *heavy), -most, most).astype(held_as)


def setup_inputs(seed: int = 0) -> dict:
    arg_keys = jax.random.split(jax.random.key(seed), 7)
    return {
        "train_gate": heavy_noise(arg_keys[0], (EXPERTS, D_MODEL, D_EXPERT), D_MODEL ** -0.5, 0.1875, ((0, 4), (1, 8)), (1, 2, 8, 2.0), jnp.float32),
        "other_gate": scatter_about(arg_keys[1], (EXPERTS, D_MODEL, D_EXPERT), (D_MODEL * 4) ** -0.5, 0.0625, ((0, 4), (1, 8))),
        "train_up": heavy_noise(arg_keys[2], (EXPERTS, D_MODEL, D_EXPERT), D_MODEL ** -0.5, 0.1875, ((0, 4), (1, 8)), (1, 2, 8, 2.0), jnp.float32),
        "other_up": scatter_about(arg_keys[3], (EXPERTS, D_MODEL, D_EXPERT), (D_MODEL * 4) ** -0.5, 0.0625, ((0, 4), (1, 8))),
        "router_weight": scatter_about(arg_keys[4], (D_MODEL, EXPERTS), D_MODEL ** -0.5, 0.125, ((0, 8), (1, 4)), jnp.float32),
        "router_gain": jnp.clip(1.0 + 0.15 * jax.random.normal(arg_keys[5], (D_MODEL,), jnp.float32), 0.25, 1.75),
    }


def reference(train_gate, other_gate, train_up, other_up, router_weight, router_gain):
    latest_gate = train_gate + other_gate.astype(jnp.float32)
    latest_up = train_up + other_up.astype(jnp.float32)
    scale_gate = jnp.max(jnp.abs(latest_gate), axis=1)
    ready_gate = (latest_gate / jnp.expand_dims(scale_gate, 1)).astype(jnp.bfloat16)
    scale_up = jnp.max(jnp.abs(latest_up), axis=1)
    ready_up = (latest_up / jnp.expand_dims(scale_up, 1)).astype(jnp.bfloat16)
    serve_router = (router_weight * router_gain[:, None]).astype(jnp.bfloat16)
    return ready_gate, ready_up, scale_gate, scale_up, serve_router
```

```python
import functools

import jax
import jax.numpy as jnp
from jax import lax
from jax.experimental import pallas as pl
from jax.experimental.pallas import tpu as pltpu
from jax.sharding import PartitionSpec as P

LANES = 128
SLOTS = 3


def exchange(
    n, held,
    train_gate, other_gate, train_up, other_up,
    ready_gate, ready_up, scale_ref,
    train_in, other_in, stage, local_max, peer_max,
    in_sem, own_sem, send_sem, recv_sem, max_send, max_recv,
):
    trains, others, readies = (train_gate, train_up), (other_gate, other_up), (ready_gate, ready_up)
    experts, rows, width = train_gate.shape
    piece = width // n
    groups = experts // held
    me = lax.axis_index("zero")
    offsets = sorted(range(1, n), key=lambda k: abs(2 * k - n))

    def loads(g):
        slot = lax.rem(g, SLOTS)
        some = pl.ds(g * held, held)
        out = []
        for t in range(2):
            out.append(pltpu.make_async_copy(trains[t].at[some], train_in.at[slot, t], in_sem.at[slot, t, 0]))
            out.append(pltpu.make_async_copy(others[t].at[some], other_in.at[slot, t], in_sem.at[slot, t, 1]))
        return out

    def max_copy(g, k):
        return pltpu.make_async_remote_copy(
            src_ref=local_max.at[g],
            dst_ref=peer_max.at[g, k - 1],
            send_sem=max_send.at[k - 1],
            recv_sem=max_recv.at[g],
            device_id={"zero": lax.rem(me + k, n)},
            device_id_type=pl.DeviceIdType.MESH,
        )

    def find_max(g):
        slot = lax.rem(g, SLOTS)
        for copy in loads(g):
            copy.wait()

        for t in range(2):
            for i in range(held):
                for at in range(0, width, LANES):
                    cols = pl.ds(at, LANES)
                    latest = train_in[slot, t, i, :, cols] + other_in[slot, t, i, :, cols].astype(jnp.float32)
                    local_max[g, t, i:i + 1, cols] = jnp.max(jnp.abs(latest), axis=0, keepdims=True)
        for k in offsets:
            max_copy(g, k).start()

    def mine(ref):
        return ref.at[:, :, pl.ds(pl.multiple_of(me * rows, LANES), rows)]

    def scale_and_send(g):
        slot = lax.rem(g, SLOTS)
        pltpu.make_async_copy(peer_max.at[g], peer_max.at[g], max_recv.at[g]).wait()

        for t in range(2):
            scales = local_max[g, t]
            for k in range(n - 1):
                scales = jnp.maximum(scales, peer_max[g, k, t])
            scale_ref[g, t] = scales
            inverses = 1.0 / scales
            for i in range(held):
                inverse = inverses[i:i + 1, :]
                for at in range(0, width, LANES):
                    cols = pl.ds(at, LANES)
                    latest = train_in[slot, t, i, :, cols] + other_in[slot, t, i, :, cols].astype(jnp.float32)
                    narrow = (latest * inverse[:, at:at + LANES]).astype(jnp.bfloat16)
                    stage[t, g * held + i, cols, :] = narrow.T
        some = pl.ds(g * held, held)
        for k in offsets:
            to = lax.rem(me + k, n)
            for t in range(2):
                pltpu.make_async_remote_copy(
                    src_ref=stage.at[t, some, pl.ds(pl.multiple_of(to * piece, 16), piece), :],
                    dst_ref=mine(readies[t]).at[some],
                    send_sem=send_sem.at[t, k - 1],
                    recv_sem=recv_sem.at[t, k - 1],
                    device_id={"zero": to},
                    device_id_type=pl.DeviceIdType.MESH,
                ).start()
        for t in range(2):
            pltpu.make_async_copy(
                stage.at[t, some, pl.ds(pl.multiple_of(me * piece, 16), piece), :],
                mine(readies[t]).at[some],
                own_sem.at[t],
            ).start()

    for g in range(min(SLOTS, groups)):
        for copy in loads(g):
            copy.start()
    barrier = pltpu.get_barrier_semaphore()
    for k in offsets:
        pl.semaphore_signal(
            barrier, inc=1, device_id={"zero": lax.rem(me + k, n)}, device_id_type=pl.DeviceIdType.MESH
        )
    pl.semaphore_wait(barrier, n - 1)
    find_max(0)

    def step(g, carry):
        @pl.when(g + 1 < groups)
        def _():
            find_max(g + 1)

        scale_and_send(g)

        @pl.when(g + SLOTS < groups)
        def _():
            for copy in loads(g + SLOTS):
                copy.start()

        return carry

    lax.fori_loop(0, groups, step, 0)

    for k in offsets:
        sent = local_max
        pltpu.make_async_copy(sent, sent, max_send.at[k - 1]).wait()
        to, source = lax.rem(me + k, n), lax.rem(me + n - k, n)
        for t in range(2):
            sent = stage.at[t, :, pl.ds(pl.multiple_of(to * piece, 16), piece), :]
            pltpu.make_async_copy(sent, sent, send_sem.at[t, k - 1]).wait()
            got = readies[t].at[:, :, pl.ds(pl.multiple_of(source * rows, LANES), rows)]
            pltpu.make_async_copy(got, got, recv_sem.at[t, k - 1]).wait()
    for t in range(2):
        pltpu.make_async_copy(mine(readies[t]), mine(readies[t]), own_sem.at[t]).wait()


def weights_by_kernel(n, held, train_gate, other_gate, train_up, other_up):
    experts, rows, width = train_gate.shape
    piece, groups = width // n, experts // held
    anywhere = pl.BlockSpec(memory_space=pltpu.MemorySpace.HBM)
    ready = jax.ShapeDtypeStruct((experts, piece, n * rows), jnp.bfloat16)
    ready_gate, ready_up, scales = pl.pallas_call(
        functools.partial(exchange, n, held),
        out_shape=(ready, ready, jax.ShapeDtypeStruct((groups, 2, held, width), jnp.float32)),
        in_specs=[anywhere] * 4,
        out_specs=(anywhere, anywhere, pl.BlockSpec(memory_space=pltpu.VMEM)),
        scratch_shapes=[
            pltpu.VMEM((SLOTS, 2, held, rows, width), jnp.float32),
            pltpu.VMEM((SLOTS, 2, held, rows, width), jnp.bfloat16),
            pltpu.VMEM((2, experts, width, rows), jnp.bfloat16),
            pltpu.VMEM((groups, 2, held, width), jnp.float32),
            pltpu.VMEM((groups, n - 1, 2, held, width), jnp.float32),
            pltpu.SemaphoreType.DMA((SLOTS, 2, 2)),
            pltpu.SemaphoreType.DMA((2,)),
            pltpu.SemaphoreType.DMA((2, n - 1)),
            pltpu.SemaphoreType.DMA((2, n - 1)),
            pltpu.SemaphoreType.DMA((n - 1,)),
            pltpu.SemaphoreType.DMA((groups,)),
        ],
        compiler_params=pltpu.CompilerParams(
            collective_id=0, has_side_effects=True, vmem_limit_bytes=56 * 2**20
        ),
    )(train_gate, other_gate, train_up, other_up)
    mine = lax.dynamic_slice_in_dim(scales, lax.axis_index("zero") * piece, piece, axis=3)
    mine = jnp.swapaxes(mine, 0, 1).reshape(2, experts, piece)
    return jnp.swapaxes(ready_gate, 1, 2), jnp.swapaxes(ready_up, 1, 2), mine[0], mine[1]


def weights_by_collectives(train_gate, other_gate, train_up, other_up):
    latest_gate = train_gate + other_gate.astype(jnp.float32)
    latest_up = train_up + other_up.astype(jnp.float32)
    scale_gate, scale_up = lax.pmax(
        (jnp.max(jnp.abs(latest_gate), axis=1), jnp.max(jnp.abs(latest_up), axis=1)), "zero"
    )
    narrow_gate, narrow_up = (
        (latest_gate / jnp.expand_dims(scale_gate, 1)).astype(jnp.bfloat16),
        (latest_up / jnp.expand_dims(scale_up, 1)).astype(jnp.bfloat16),
    )
    ready_gate, ready_up = (
        lax.all_to_all(narrow_gate, "zero", split_axis=2, concat_axis=1, tiled=True),
        lax.all_to_all(narrow_up, "zero", split_axis=2, concat_axis=1, tiled=True),
    )
    scale_gate = lax.dynamic_slice_in_dim(
        scale_gate, lax.axis_index("zero") * ready_gate.shape[2], ready_gate.shape[2], axis=1
    )
    scale_up = lax.dynamic_slice_in_dim(
        scale_up, lax.axis_index("zero") * ready_up.shape[2], ready_up.shape[2], axis=1
    )
    return ready_gate, ready_up, scale_gate, scale_up


def on_device(n, train_gate, other_gate, train_up, other_up, router_weight, router_gain):
    part_router = (router_weight * router_gain[:, None]).astype(jnp.bfloat16)
    row_router = lax.all_gather(part_router, "zero", axis=0, tiled=True)
    serve_router = lax.all_gather(row_router, "bank", axis=1, tiled=True)
    experts, rows, width = train_gate.shape
    held = 2 if experts % 2 == 0 else 1
    whole_tiles = rows % LANES == 0 and width % LANES == 0 and (width // n) % 16 == 0
    staged = 4 * experts * rows * width + SLOTS * held * 12 * rows * width
    if n > 1 and whole_tiles and staged <= 48 * 2**20:
        weights = weights_by_kernel(n, held, train_gate, other_gate, train_up, other_up)
    else:
        weights = weights_by_collectives(train_gate, other_gate, train_up, other_up)
    return (*weights, serve_router)


def solution(mesh):
    return jax.shard_map(
        functools.partial(on_device, mesh.shape["zero"]),
        mesh=mesh,
        in_specs=(
            P("bank", "zero", None),
            P("bank", "zero", None),
            P("bank", "zero", None),
            P("bank", "zero", None),
            P("zero", "bank"),
            P("zero"),
        ),
        out_specs=(
            P("bank", None, "zero"),
            P("bank", None, "zero"),
            P("bank", "zero"),
            P("bank", "zero"),
            P(),
        ),
        check_vma=False,
    )
```
